32 devices in a mesh: seq: 4 (over x, core), tensor: 8 (over z, y).
Axes of the slice: x: 2, y: 2, z: 4, core: 2. Of those that a mesh axis runs over, the one named last changes fastest.
Arguments:
- token_ids: int32 [2, 7], replicated, may hold values from 0 to 131071
- cache_lengths: int32 [7], replicated, may hold values from 1 to 5118
- embed_table: bfloat16 [131072, 1024], P('seq', 'tensor'), may hold values from -64 to 64
- attn_gain: float32 [1024], replicated, may hold values from 0.1 to 1.9
- final_gain: float32 [1024], replicated, may hold values from 0.1 to 1.9
- w_qkv: bfloat16 [1024, 3, 1024], P(None, None, 'tensor'), may hold values from -0.1875 to 0.1875
- w_out: bfloat16 [1024, 1024], P('tensor'), may hold values from -0.1875 to 0.1875
- cache_keys: bfloat16 [7, 5120, 1024], P(None, 'seq', 'tensor'), may hold values from -300 to 300
- cache_values: bfloat16 [7, 5120, 1024], P(None, 'seq', 'tensor'), may hold values from -24 to 24
Outputs:
- hidden: bfloat16 [2, 7, 1024], P(None, None, 'tensor')
- new_kv: bfloat16 [2, 2, 7, 1024], P(None, None, None, 'tensor')
- logprobs: float32 [2, 7, 131072], P(None, None, ('seq', 'tensor'))
The draws below stay inside these ranges and needn't reach their ends.
All inputs are finite; a program needn't handle non-finite values.
Results may differ from the reference program's by a relative error of at most 0.0085.
The reference program's roundings to bfloat16 on the way (of `embedded`, `normed`, `queries`, `attended` and `gated_rows`) count: a program that leaves them out, or rounds other values in their place, can miss the bound.
Values may be sent and summed in bfloat16 or wider, within the bound.
A program may use at most 64 MiB of HBM per device.

```python
import math
import jax
import jax.numpy as jnp
from jax import lax

HD = 128
D = 1024
V = 131072
STREAMS = 7
CTX = 5120


def draw_embed_table(key, part):
    base_key = jax.random.fold_in(jax.random.fold_in(key, 11), 0)
    table = 0.25 * jnp.clip(jax.random.normal(base_key, (V, D), jnp.float32), -4.0, 4.0)
    position = jnp.arange(D, dtype=jnp.float32) / (D - 1)
    vocab_position = jnp.arange(V, dtype=jnp.float32) / (V - 1)
    row_rise = jnp.exp(vocab_position * math.log(3.0))[:, None]
    column_scale = jnp.exp(position * math.log(4.0))
    row_scale = row_rise
    table = table * row_scale * column_scale[None, :]
    return table.astype(jnp.bfloat16)


def draw_cache_keys(key, part):
    base_key = jax.random.fold_in(jax.random.fold_in(key, 23), 0)
    keys_drawn = jnp.clip(jax.random.normal(base_key, (STREAMS, CTX, D), jnp.float32), -5.0, 5.0)
    return keys_drawn.astype(jnp.bfloat16)


def with_ends(entries, stream_key, low, largest):
    extent = entries.shape
    index_at = [jax.random.randint(jax.random.fold_in(stream_key, axis), (), 0, extent[axis]) for axis in range(len(extent))]
    entries = entries.at[tuple(index_at)].set(low)
    longest = extent.index(max(extent))
    index_at[longest] = (index_at[longest] + 1) % extent[longest]
    return entries.at[tuple(index_at)].set(largest)


def shard_levels(rng, dims, shards, low, high):
    gain, own = 1.0, jax.random.fold_in(rng, 6)
    for axis_at, parts in shards:
        heights = jnp.exp(jax.random.uniform(jax.random.fold_in(own, axis_at), (parts,), jnp.float32, low / len(shards), high / len(shards)))
        gain = gain * jnp.repeat(heights, dims[axis_at] // parts).reshape([-1 if axis == axis_at else 1 for axis in range(len(dims))])
    return gain


def noise(own_key, extent, width, most, cuts=(), kind=jnp.bfloat16):
    entries = jax.random.normal(own_key, extent, jnp.float32) * width
    if len(cuts) > 0:
        entries = shard_levels(own_key, extent, cuts, -0.22, 0.18) * entries
    return jnp.clip(entries, min=-most, max=most).astype(kind)


def setup_inputs(seed: int = 0) -> dict:
    keys = jax.random.split(jax.random.key(seed), 10)
    return {
        "token_ids": with_ends(jax.random.randint(keys[0], (2, STREAMS), 0, V), jax.random.fold_in(keys[0], 1), 0, V - 1).astype(jnp.int32),
        "cache_lengths": with_ends(jax.random.randint(keys[1], (STREAMS,), 1, CTX - 1), jax.random.fold_in(keys[1], 1), 1, (CTX - 1) - 1).astype(jnp.int32),
        "embed_table": draw_embed_table(jax.random.fold_in(keys[9], 71), 0),
        "attn_gain": jnp.clip(1.0 + 0.18 * jax.random.normal(keys[3], (D,), jnp.float32), 0.1, 1.9),
        "final_gain": jnp.clip(1.0 + 0.18 * jax.random.normal(keys[4], (D,), jnp.float32), 0.1, 1.9),
        "w_qkv": noise(keys[5], (D, 3, D), D ** -0.5, 0.1875, ((2, 8),)),
        "w_out": noise(keys[6], (D, D), D ** -0.5, 0.1875, ((0, 8),)),
        "cache_keys": draw_cache_keys(jax.random.fold_in(keys[9], 71), 0),
        "cache_values": noise(keys[8], (STREAMS, CTX, D), 4.0, 24.0, ((1, 4), (2, 8))),
    }


epsilon = 1e-05
logit_gain = 2.0

def rotate(vector, positions):
    half_size = vector.shape[-1] // 2
    frequency = 10000.0 ** (-(jnp.arange(half_size, dtype=jnp.float32) * 2.0 / vector.shape[-1]))
    angles = positions.astype(jnp.float32)[..., None] * frequency
    cosine_term = jnp.cos(angles)[:, :, None, :]
    sine_term = jnp.sin(angles)[:, :, None, :]
    first_half = vector[..., :half_size]
    second_half = vector[..., half_size:]
    return jnp.concatenate([first_half * cosine_term - second_half * sine_term, first_half * sine_term + second_half * cosine_term], -1)

def reference(token_ids, cache_lengths, embed_table, attn_gain, final_gain, w_qkv, w_out, cache_keys, cache_values):
    heads = D // HD
    streams = token_ids.shape[1]
    embedded = embed_table[token_ids]
    embed_float = embedded.astype(jnp.float32)
    normed = (embed_float * lax.rsqrt(lax.optimization_barrier(jnp.mean(embed_float * embed_float, -1, keepdims=True)) + epsilon) * attn_gain).astype(jnp.bfloat16)
    projected = jnp.einsum('sbd,dcf->sbcf', normed.astype(jnp.float32), w_qkv.astype(jnp.float32), precision=lax.Precision.HIGHEST)
    head_shape = (2, streams, heads, HD)
    positions = cache_lengths[None, :] + jnp.arange(2, dtype=jnp.int32)[:, None]
    queries = rotate(projected[:, :, 0].reshape(head_shape), positions).astype(jnp.bfloat16)
    new_keys = rotate(projected[:, :, 1].reshape(head_shape), positions).astype(jnp.bfloat16)
    new_values = projected[:, :, 2].reshape(head_shape).astype(jnp.bfloat16)
    new_kv = jnp.stack([new_keys.reshape(2, streams, D), new_values.reshape(2, streams, D)])
    inverse = HD ** (-0.5)
    allowed = (jnp.arange(2)[None, :] <= jnp.arange(2)[:, None])[:, None, :]

    def attend_stream(packed):
        query_rows, key_rows, value_rows, length, fresh_keys, fresh_values = packed
        key_rows = key_rows.reshape(CTX, heads, HD).astype(jnp.float32)
        value_rows = value_rows.reshape(CTX, heads, HD).astype(jnp.float32)
        query_float = query_rows.astype(jnp.float32)
        cached = jnp.einsum('she,jhe->shj', query_float, key_rows, precision=lax.Precision.HIGHEST) * inverse
        fresh = jnp.einsum('she,the->sht', query_float, fresh_keys.astype(jnp.float32), precision=lax.Precision.HIGHEST) * inverse
        visible = jnp.broadcast_to((jnp.arange(CTX) < length)[None, None, :], cached.shape)
        scores = jnp.concatenate([cached, fresh], -1)
        mask_all = jnp.concatenate([visible, jnp.broadcast_to(allowed, fresh.shape)], -1)
        highest = lax.optimization_barrier(jnp.max(jnp.where(mask_all, scores, -1e+30), -1, keepdims=True))
        weights = jnp.where(mask_all, jnp.exp(scores - highest), 0.0)
        all_values = jnp.concatenate([value_rows, fresh_values.astype(jnp.float32)], 0)
        numerator = jnp.einsum('shj,jhe->she', weights, all_values, precision=lax.Precision.HIGHEST)
        return numerator / lax.optimization_barrier(jnp.sum(weights, -1))[..., None]
    attended = lax.map(attend_stream, (jnp.transpose(queries, (1, 0, 2, 3)), cache_keys, cache_values, cache_lengths, jnp.transpose(new_keys, (1, 0, 2, 3)), jnp.transpose(new_values, (1, 0, 2, 3))))
    attended = jnp.transpose(attended, (1, 0, 2, 3)).astype(jnp.bfloat16).reshape(2 * streams, D)
    mixed_rows = jnp.dot(attended, w_out, preferred_element_type=jnp.float32).reshape(2, streams, D)
    hidden = (embed_float + mixed_rows).astype(jnp.bfloat16)
    hidden_float = hidden.astype(jnp.float32)
    factor = lax.rsqrt(lax.optimization_barrier(jnp.mean(hidden_float * hidden_float, -1)) + epsilon) * (logit_gain / jnp.sqrt(jnp.float32(D)))
    gated_rows = (hidden_float * final_gain).astype(jnp.bfloat16).reshape(2 * streams, D)
    logits = lax.dot_general(gated_rows, embed_table, (((1,), (1,)), ((), ())), preferred_element_type=jnp.float32)
    logits = logits * factor.reshape(2 * streams, 1)
    highest = lax.optimization_barrier(jnp.max(logits, -1, keepdims=True))
    logprobs = logits - (highest + jnp.log(lax.optimization_barrier(jnp.sum(jnp.exp(logits - highest), -1, keepdims=True))))
    return (hidden, new_kv, logprobs.reshape(2, streams, V))
```

```python
import functools
import math

import numpy as np

import jax
import jax.numpy as jnp
from jax import lax
from jax.experimental import pallas as pl
from jax.experimental.pallas import tpu as pltpu
from jax.sharding import PartitionSpec as P

HD = 128
ROWS = 16
TILE = 16
BF = jnp.bfloat16
F32 = jnp.float32

epsilon = 1e-05
logit_gain = 2.0


def nt_dot(a, b):
    return lax.dot_general(a, b, (((1,), (1,)), ((), ())), preferred_element_type=F32)


def local_kernel(streams, tok_ref, len_ref, freq_ref, table_hbm, pick_ref, lens_ref, cos_ref, sin_ref, blocks, sem):
    first = lax.axis_index("seq") * table_hbm.shape[0]
    last = table_hbm.shape[0] - 1
    lines = []
    copies = []
    for b in range(streams):
        for s in range(2):
            at = tok_ref[s, b] - first
            inside = (at >= 0) & (at <= last)
            safe = jnp.clip(at, 0, last)
            base = lax.div(safe, TILE) * TILE
            copy = pltpu.make_async_copy(
                table_hbm.at[pl.ds(pl.multiple_of(base, TILE), TILE)],
                blocks.at[2 * b + s],
                sem.at[2 * b + s],
            )
            copy.start()
            copies.append(copy)
            lines.append(jnp.where(inside, safe - base, -1))
    row = lax.broadcasted_iota(jnp.int32, (ROWS, HD), 0)
    lane = lax.broadcasted_iota(jnp.int32, (ROWS, HD), 1)
    lens = jnp.ones((ROWS, HD), jnp.int32)
    for b in range(streams):
        lens = jnp.where(lax.div(row, 2) == b, len_ref[b], lens)
    lens_ref[...] = lens
    angle = (lens + lax.rem(row, 2)).astype(F32) * freq_ref[...]
    cos_ref[...] = jnp.cos(angle)
    sine = jnp.sin(angle)
    sin_ref[...] = jnp.where(lane < HD // 2, -sine, sine)
    picked = jnp.zeros((ROWS, HD), F32)
    for i in range(2 * streams):
        copies[i].wait()
        line = jnp.where(row == lines[i], blocks[i].astype(F32), 0.0)
        picked = jnp.where(row == i, jnp.sum(line, 0, keepdims=True), picked)
    pick_ref[...] = picked.astype(BF)


def kernel(
    n_seq, n_tensor, streams, model_width,
    pick_ref, lens_ref, cos_ref, sin_ref, again_ref, fgain_ref, table_hbm, wqkv_hbm, wout_hbm, keys_hbm, values_hbm,
    hidden_ref, newkv_ref, logp_ref,
    table, wqkv, wout, keys, values,
    pick_all, emb_all, flash_all, mix_out, mix_all, sq_all, lsa_all, lsb_all,
    pair_out, pair_in, own, far_out, far_in, logits,
    dma_sem,
    pick_s, pick_r, emb_s, emb_r, flash_s, flash_r, mix_s, mix_r, sq_s, sq_r,
    lsa_s, lsa_r, lsb_s, lsb_r, pair_s, pair_r, far_s, far_r,
):
    me_s = lax.axis_index("seq")
    me_t = lax.axis_index("tensor")
    vocab_rows = table.shape[0]
    slot_count = keys.shape[1]
    groups = n_tensor // 2
    share = vocab_rows // n_tensor

    parts = 4
    piece = vocab_rows // parts
    loads = [
        pltpu.make_async_copy(
            table_hbm.at[pl.ds(i * piece, piece)], table.at[pl.ds(i * piece, piece)], dma_sem.at[i]
        )
        for i in range(parts)
    ]
    load_wqkv = pltpu.make_async_copy(wqkv_hbm, wqkv, dma_sem.at[parts])
    load_keys = pltpu.make_async_copy(keys_hbm, keys, dma_sem.at[parts + 1])
    load_values = pltpu.make_async_copy(values_hbm, values, dma_sem.at[parts + 2])
    load_wout = pltpu.make_async_copy(wout_hbm, wout, dma_sem.at[parts + 3])
    for load in loads + [load_wqkv, load_keys, load_values, load_wout]:
        load.start()

    def seq_peer(k):
        return lax.rem(me_s + k, n_seq)

    def tensor_peer(k):
        return lax.rem(me_t + k, n_tensor)

    barrier = pltpu.get_barrier_semaphore()
    for k in range(1, n_seq):
        pl.semaphore_signal(
            barrier, inc=1, device_id=(seq_peer(k), me_t), device_id_type=pl.DeviceIdType.MESH
        )
    for k in range(1, n_tensor):
        pl.semaphore_signal(
            barrier, inc=1, device_id=(me_s, tensor_peer(k)), device_id_type=pl.DeviceIdType.MESH
        )

    def exchange(src_of, dst, send, recv, axis):
        count = n_seq if axis == "seq" else n_tensor
        mine = me_s if axis == "seq" else me_t
        copies = []
        for k in range(1, count):
            if axis == "seq":
                peer = seq_peer(k)
                target = (peer, me_t)
            else:
                peer = tensor_peer(k)
                target = (me_s, peer)
            copy = pltpu.make_async_remote_copy(
                src_ref=src_of(peer),
                dst_ref=dst.at[mine],
                send_sem=send.at[k],
                recv_sem=recv.at[k],
                device_id=target,
                device_id_type=pl.DeviceIdType.MESH,
            )
            copy.start()
            copies.append(copy)
        return copies

    row = lax.broadcasted_iota(jnp.int32, (ROWS, HD), 0)
    lane = lax.broadcasted_iota(jnp.int32, (ROWS, HD), 1)
    stream = lax.div(row, 2)
    step = lax.rem(row, 2)
    lens = lens_ref[...]
    cosine = cos_ref[...]
    sine = sin_ref[...]
    pick_all[me_s] = pick_ref[...]
    pl.semaphore_wait(barrier, n_seq - 1 + n_tensor - 1)
    sent = exchange(lambda peer: pick_ref, pick_all, pick_s, pick_r, "seq")
    for copy in sent:
        copy.wait_recv()
    embed = pick_all[0].astype(F32)
    for i in range(1, n_seq):
        embed = embed + pick_all[i].astype(F32)
    emb_all[me_t] = embed.astype(BF)
    more = exchange(lambda peer: emb_all.at[me_t], emb_all, emb_s, emb_r, "tensor")
    load_wqkv.wait()
    for load in loads:
        load.wait()
    for copy in more:
        copy.wait_recv()
    sent += more
    squares = jnp.zeros((ROWS, HD), F32)
    for i in range(n_tensor):
        part = emb_all[i].astype(F32)
        squares = squares + part * part
    norm = lax.rsqrt(jnp.sum(squares, -1, keepdims=True) / model_width + epsilon)
    normed = jnp.concatenate(
        [
            (emb_all[i].astype(F32) * norm * again_ref[:, i * HD : (i + 1) * HD]).astype(BF)
            for i in range(n_tensor)
        ],
        1,
    )
    projected = [jnp.dot(normed, wqkv[c], preferred_element_type=F32) for c in range(3)]

    def rotate(x):
        return x * cosine + pltpu.roll(x, HD // 2, 1) * sine

    queries = rotate(projected[0]).astype(BF)
    new_keys = rotate(projected[1]).astype(BF)
    new_values = projected[2].astype(BF)
    for b in range(streams):
        newkv_ref[0, b] = new_keys[2 * b : 2 * b + 2]
        newkv_ref[1, b] = new_values[2 * b : 2 * b + 2]

    inverse = HD ** (-0.5)
    load_keys.wait()
    wide_stream = lax.div(lax.broadcasted_iota(jnp.int32, (ROWS, slot_count), 0), 2)
    scores = jnp.zeros((ROWS, slot_count), F32)
    for b in range(streams):
        scores = jnp.where(wide_stream == b, nt_dot(queries, keys[b]), scores)
    scores = scores * inverse
    slot = me_s * slot_count + lax.broadcasted_iota(jnp.int32, (ROWS, slot_count), 1)
    visible = slot < lens[:, :1]
    top = jnp.max(jnp.where(visible, scores, -1e30), -1, keepdims=True)
    weights = jnp.where(visible, jnp.exp(scores - top), 0.0)
    total = jnp.sum(weights, -1, keepdims=True)
    high = weights.astype(BF)
    low = (weights - high.astype(F32)).astype(BF)
    both = jnp.concatenate([high, low], 0)
    load_values.wait()
    gathered = jnp.zeros((ROWS, HD), F32)
    for b in range(streams):
        twin = jnp.dot(both, values[b], preferred_element_type=F32)
        gathered = jnp.where(stream == b, twin[:ROWS] + twin[ROWS:], gathered)
    flash_all[me_s, :, :HD] = gathered
    flash_all[me_s, :, HD:] = jnp.where(lane < HD // 2, top, total)
    more = exchange(lambda peer: flash_all.at[me_s], flash_all, flash_s, flash_r, "seq")

    def twice(x, s):
        return jnp.where(step == s, x, pltpu.roll(x, 1 if s == 0 else ROWS - 1, 0))

    qf = queries.astype(F32)
    kf = new_keys.astype(F32)
    vf = new_values.astype(F32)
    fresh0 = jnp.sum(qf * twice(kf, 0), -1, keepdims=True) * inverse
    fresh1 = jnp.sum(qf * twice(kf, 1), -1, keepdims=True) * inverse
    second = step[:, :1] == 1
    fresh1 = jnp.where(second, fresh1, -1e30)
    fresh_top = jnp.maximum(fresh0, fresh1)
    for copy in more:
        copy.wait_recv()
    sent += more
    tops = [flash_all[i, :, HD : HD + 1] for i in range(n_seq)]
    best = fresh_top
    for item in tops:
        best = jnp.maximum(best, item)
    w0 = jnp.exp(fresh0 - best)
    w1 = jnp.where(second, jnp.exp(fresh1 - best), 0.0)
    numerator = w0 * twice(vf, 0) + w1 * twice(vf, 1)
    denominator = w0 + w1
    for i in range(n_seq):
        factor = jnp.exp(tops[i] - best)
        numerator = numerator + flash_all[i, :, :HD] * factor
        denominator = denominator + flash_all[i, :, 2 * HD - 1 : 2 * HD] * factor
    attended = (numerator / denominator).astype(BF)

    load_wout.wait()
    for i in range(n_tensor):
        mix_out[i] = jnp.dot(
            attended, wout[:, i * HD : (i + 1) * HD], preferred_element_type=F32
        )
    more = exchange(lambda peer: mix_out.at[peer], mix_all, mix_s, mix_r, "tensor")
    mix_all[me_t] = mix_out[me_t]
    for copy in more:
        copy.wait_recv()
    sent += more
    mixed = mix_all[0]
    for i in range(1, n_tensor):
        mixed = mixed + mix_all[i]
    hidden = (emb_all[me_t].astype(F32) + mixed).astype(BF)
    for b in range(streams):
        hidden_ref[b] = hidden[2 * b : 2 * b + 2]
    hf = hidden.astype(F32)
    diagonal = row == lane

    def to_lanes(column):
        return jnp.sum(jnp.where(diagonal, column, 0.0), 0, keepdims=True)

    def to_rows(line, shift):
        return jnp.sum(jnp.where(lane == row + shift, line, 0.0), -1, keepdims=True)

    gated = (hf * fgain_ref[me_t]).astype(BF)

    pair = lax.rem(me_t, 2)
    group = lax.div(me_t, 2)
    partner = me_t + 1 - 2 * pair

    def part_logits(owner):
        return nt_dot(gated, table[pl.ds(pl.multiple_of(owner * share, share), share), :])

    pair_copies = []
    for k in range(1, groups + 1):
        g = lax.rem(group + k, groups)
        pair_out[k - 1] = part_logits(2 * g + 1 - pair).astype(BF)
        copy = pltpu.make_async_remote_copy(
            src_ref=pair_out.at[k - 1],
            dst_ref=pair_in.at[k - 1],
            send_sem=pair_s.at[k - 1],
            recv_sem=pair_r.at[k - 1],
            device_id=(me_s, partner),
            device_id_type=pl.DeviceIdType.MESH,
        )
        copy.start()
        pair_copies.append(copy)
    sq_all[me_t] = to_lanes(jnp.sum(hf * hf, -1, keepdims=True))
    sq_copies = exchange(lambda peer: sq_all.at[me_t], sq_all, sq_s, sq_r, "tensor")
    for k in range(1, groups + 1):
        g = lax.rem(group + k, groups)
        own[k - 1] = part_logits(2 * g + pair)
    far_copies = []
    for k in range(1, groups):
        g = lax.rem(group + k, groups)
        pair_copies[k - 1].wait_recv()
        far_out[k - 1] = (own[k - 1] + pair_in[k - 1].astype(F32)).astype(BF)
        copy = pltpu.make_async_remote_copy(
            src_ref=far_out.at[k - 1],
            dst_ref=far_in.at[k - 1],
            send_sem=far_s.at[k - 1],
            recv_sem=far_r.at[k - 1],
            device_id=(me_s, 2 * g + pair),
            device_id_type=pl.DeviceIdType.MESH,
        )
        copy.start()
        far_copies.append(copy)
    for copy in sq_copies:
        copy.wait_recv()
    all_squares = sq_all[0]
    for i in range(1, n_tensor):
        all_squares = all_squares + sq_all[i]
    scale = lax.rsqrt(to_rows(all_squares, 0) / model_width + epsilon) * (
        logit_gain / math.sqrt(model_width)
    )
    pair_copies[groups - 1].wait_recv()
    value = own[groups - 1] + pair_in[groups - 1].astype(F32)
    for k in range(1, groups):
        far_copies[k - 1].wait_recv()
        value = value + far_in[k - 1].astype(F32)
    value = value * scale
    logits[...] = value
    high_here = jnp.max(value, -1, keepdims=True)
    sum_here = jnp.sum(jnp.exp(value - high_here), -1, keepdims=True)

    def packed(top_column, sum_column):
        return jnp.sum(
            jnp.where(diagonal, top_column, jnp.where(lane == row + ROWS, sum_column, 0.0)),
            0,
            keepdims=True,
        )

    def joined(store, count):
        highs = [to_rows(store[i], 0) for i in range(count)]
        sums = [to_rows(store[i], ROWS) for i in range(count)]
        peak = highs[0]
        for item in highs[1:]:
            peak = jnp.maximum(peak, item)
        summed = sums[0] * jnp.exp(highs[0] - peak)
        for i in range(1, count):
            summed = summed + sums[i] * jnp.exp(highs[i] - peak)
        return peak, summed

    lsa_all[me_s] = packed(high_here, sum_here)
    more = exchange(lambda peer: lsa_all.at[me_s], lsa_all, lsa_s, lsa_r, "seq")
    for copy in more:
        copy.wait_recv()
    sent += more
    lsb_all[me_t] = packed(*joined(lsa_all, n_seq))
    more = exchange(lambda peer: lsb_all.at[me_t], lsb_all, lsb_s, lsb_r, "tensor")
    for copy in more:
        copy.wait_recv()
    sent += more
    peak, summed = joined(lsb_all, n_tensor)
    answer = logits[...] - (peak + jnp.log(summed))
    for b in range(streams):
        logp_ref[b] = answer[2 * b : 2 * b + 2]
    for copy in sent + pair_copies + sq_copies + far_copies:
        copy.wait_send()


def body(
    n_seq, n_tensor,
    token_ids, cache_lengths, embed_table, attn_gain, final_gain, w_qkv, w_out, cache_keys, cache_values,
):
    streams = token_ids.shape[1]
    vocab_rows, width = embed_table.shape
    model_width = attn_gain.shape[0]
    share = vocab_rows // n_tensor
    groups = n_tensor // 2
    slot_count = cache_keys.shape[1]
    assert width == HD and 2 * streams <= ROWS and n_tensor % 2 == 0
    half = HD // 2
    powers = 10000.0 ** (-(np.arange(half, dtype=np.float64) * 2.0 / HD))
    freq = jnp.asarray(np.concatenate([powers, powers])[None].astype(np.float32))
    vmem = pl.BlockSpec(memory_space=pltpu.VMEM)
    smem = pl.BlockSpec(memory_space=pltpu.SMEM)
    hbm = pl.BlockSpec(memory_space=pl.ANY)
    sems = lambda n: pltpu.SemaphoreType.DMA((n,))
    row_shape = lambda dtype: jax.ShapeDtypeStruct((ROWS, HD), dtype)
    picked, lens, cosine, sine = pl.pallas_call(
        functools.partial(local_kernel, streams),
        out_shape=(row_shape(BF), row_shape(jnp.int32), row_shape(F32), row_shape(F32)),
        in_specs=[smem, smem, vmem, hbm],
        out_specs=(vmem,) * 4,
        scratch_shapes=[pltpu.VMEM((2 * streams, TILE, HD), BF), sems(2 * streams)],
        compiler_params=pltpu.CompilerParams(vmem_limit_bytes=60 * 1024 * 1024),
        name="rows",
    )(token_ids, cache_lengths, freq, embed_table)
    hidden, new_kv, logprobs = pl.pallas_call(
        functools.partial(kernel, n_seq, n_tensor, streams, model_width),
        out_shape=(
            jax.ShapeDtypeStruct((streams, 2, HD), BF),
            jax.ShapeDtypeStruct((2, streams, 2, HD), BF),
            jax.ShapeDtypeStruct((streams, 2, share), F32),
        ),
        in_specs=[vmem] * 6 + [hbm] * 5,
        out_specs=(vmem, vmem, vmem),
        scratch_shapes=[
            pltpu.VMEM((vocab_rows, HD), BF),
            pltpu.VMEM((3, model_width, HD), BF),
            pltpu.VMEM((HD, model_width), BF),
            pltpu.VMEM((streams, slot_count, HD), BF),
            pltpu.VMEM((streams, slot_count, HD), BF),
            pltpu.VMEM((n_seq, ROWS, HD), BF),
            pltpu.VMEM((n_tensor, ROWS, HD), BF),
            pltpu.VMEM((n_seq, ROWS, 2 * HD), F32),
            pltpu.VMEM((n_tensor, ROWS, HD), F32),
            pltpu.VMEM((n_tensor, ROWS, HD), F32),
            pltpu.VMEM((n_tensor, 1, HD), F32),
            pltpu.VMEM((n_seq, 1, HD), F32),
            pltpu.VMEM((n_tensor, 1, HD), F32),
            pltpu.VMEM((groups, ROWS, share), BF),
            pltpu.VMEM((groups, ROWS, share), BF),
            pltpu.VMEM((groups, ROWS, share), F32),
            pltpu.VMEM((groups, ROWS, share), BF),
            pltpu.VMEM((groups, ROWS, share), BF),
            pltpu.VMEM((ROWS, share), F32),
            sems(8),
            sems(n_seq), sems(n_seq), sems(n_tensor), sems(n_tensor),
            sems(n_seq), sems(n_seq), sems(n_tensor), sems(n_tensor),
            sems(n_tensor), sems(n_tensor),
            sems(n_seq), sems(n_seq), sems(n_tensor), sems(n_tensor),
            sems(groups), sems(groups), sems(groups), sems(groups),
        ],
        compiler_params=pltpu.CompilerParams(
            collective_id=0, has_side_effects=True, vmem_limit_bytes=60 * 1024 * 1024
        ),
        name="decode",
    )(
        picked,
        lens,
        cosine,
        sine,
        attn_gain.reshape(1, model_width),
        final_gain.reshape(n_tensor, 1, HD),
        embed_table,
        jnp.transpose(w_qkv, (1, 0, 2)),
        w_out,
        cache_keys,
        cache_values,
    )
    return (
        jnp.transpose(hidden, (1, 0, 2)),
        jnp.transpose(new_kv, (0, 2, 1, 3)),
        jnp.transpose(logprobs, (1, 0, 2)),
    )


def solution(mesh):
    in_specs = (
        P(),
        P(),
        P("seq", "tensor"),
        P(),
        P(),
        P(None, None, "tensor"),
        P("tensor", None),
        P(None, "seq", "tensor"),
        P(None, "seq", "tensor"),
    )
    out_specs = (
        P(None, None, "tensor"),
        P(None, None, None, "tensor"),
        P(None, None, ("seq", "tensor")),
    )
    return jax.shard_map(
        functools.partial(body, mesh.shape["seq"], mesh.shape["tensor"]),
        mesh=mesh, in_specs=in_specs, out_specs=out_specs, check_vma=False,
    )
```

```python
import functools
import math

import numpy as np

import jax
import jax.numpy as jnp
from jax import lax
from jax.experimental import pallas as pl
from jax.experimental.pallas import tpu as pltpu
from jax.sharding import PartitionSpec as P

HD = 128
ROWS = 16
TILE = 16
HALVES = 2
BF = jnp.bfloat16
F32 = jnp.float32

epsilon = 1e-05
logit_gain = 2.0


def nt_dot(a, b):
    return lax.dot_general(a, b, (((1,), (1,)), ((), ())), preferred_element_type=F32)


def local_kernel(streams, tok_ref, len_ref, freq_ref, table_hbm, pick_ref, lens_ref, cos_ref, sin_ref, blocks, sem):
    first = lax.axis_index("seq") * table_hbm.shape[0]
    last = table_hbm.shape[0] - 1
    lines = []
    copies = []
    for b in range(streams):
        for s in range(2):
            at = tok_ref[s, b] - first
            inside = (at >= 0) & (at <= last)
            safe = jnp.clip(at, 0, last)
            base = lax.div(safe, TILE) * TILE
            copy = pltpu.make_async_copy(
                table_hbm.at[pl.ds(pl.multiple_of(base, TILE), TILE)],
                blocks.at[2 * b + s],
                sem.at[2 * b + s],
            )
            copy.start()
            copies.append(copy)
            lines.append(jnp.where(inside, safe - base, -1))
    row = lax.broadcasted_iota(jnp.int32, (ROWS, HD), 0)
    lane = lax.broadcasted_iota(jnp.int32, (ROWS, HD), 1)
    lens = jnp.ones((ROWS, HD), jnp.int32)
    for b in range(streams):
        lens = jnp.where(lax.div(row, 2) == b, len_ref[b], lens)
    lens_ref[...] = lens
    angle = (lens + lax.rem(row, 2)).astype(F32) * freq_ref[...]
    cos_ref[...] = jnp.cos(angle)
    sine = jnp.sin(angle)
    sin_ref[...] = jnp.where(lane < HD // 2, -sine, sine)
    picked = jnp.zeros((ROWS, HD), F32)
    for i in range(2 * streams):
        copies[i].wait()
        line = jnp.where(row == lines[i], blocks[i].astype(F32), 0.0)
        picked = jnp.where(row == i, jnp.sum(line, 0, keepdims=True), picked)
    pick_ref[...] = picked.astype(BF)


def kernel(
    n_seq, n_tensor, streams, model_width,
    pick_ref, lens_ref, cos_ref, sin_ref, again_ref, fgain_ref, table_hbm, wqkv_hbm, wout_hbm, keys_hbm, values_hbm,
    hidden_ref, fresh_k_ref, fresh_v_ref, lse_ref, logits_hbm,
    table, wqkv, wout, keys, values,
    pick_all, emb_all, flash_all, mix_out, mix_all, sq_all, ls_all,
    pair_out, pair_in, own, far_out, far_in, logits,
    dma_sem,
    pick_s, pick_r, emb_s, emb_r, flash_s, flash_r, mix_s, mix_r, sq_s, sq_r,
    ls_s, ls_r, pair_s, pair_r, far_s, far_r,
):
    me_s = lax.axis_index("seq")
    me_t = lax.axis_index("tensor")
    vocab_rows = table.shape[0]
    slot_count = keys.shape[1]
    groups = n_tensor // 2
    share = vocab_rows // n_tensor

    parts = 4
    piece = vocab_rows // parts
    loads = [
        pltpu.make_async_copy(
            table_hbm.at[pl.ds(i * piece, piece)], table.at[pl.ds(i * piece, piece)], dma_sem.at[i]
        )
        for i in range(parts)
    ]
    load_wqkv = pltpu.make_async_copy(wqkv_hbm, wqkv, dma_sem.at[parts])
    load_keys = pltpu.make_async_copy(keys_hbm, keys, dma_sem.at[parts + 1])
    load_values = pltpu.make_async_copy(values_hbm, values, dma_sem.at[parts + 2])
    load_wout = pltpu.make_async_copy(wout_hbm, wout, dma_sem.at[parts + 3])
    for load in loads + [load_wqkv, load_keys, load_values, load_wout]:
        load.start()

    def seq_peer(k):
        return lax.rem(me_s + k, n_seq)

    def tensor_peer(k):
        return lax.rem(me_t + k, n_tensor)

    barrier = pltpu.get_barrier_semaphore()
    for k in range(1, n_seq):
        pl.semaphore_signal(
            barrier, inc=1, device_id=(seq_peer(k), me_t), device_id_type=pl.DeviceIdType.MESH
        )
    for k in range(1, n_tensor):
        pl.semaphore_signal(
            barrier, inc=1, device_id=(me_s, tensor_peer(k)), device_id_type=pl.DeviceIdType.MESH
        )

    def exchange(src_of, dst, send, recv, axis):
        count = n_seq if axis == "seq" else n_tensor
        mine = me_s if axis == "seq" else me_t
        copies = []
        for k in range(1, count):
            if axis == "seq":
                peer = seq_peer(k)
                target = (peer, me_t)
            else:
                peer = tensor_peer(k)
                target = (me_s, peer)
            copy = pltpu.make_async_remote_copy(
                src_ref=src_of(peer),
                dst_ref=dst.at[mine],
                send_sem=send.at[k],
                recv_sem=recv.at[k],
                device_id=target,
                device_id_type=pl.DeviceIdType.MESH,
            )
            copy.start()
            copies.append(copy)
        return copies

    row = lax.broadcasted_iota(jnp.int32, (ROWS, HD), 0)
    lane = lax.broadcasted_iota(jnp.int32, (ROWS, HD), 1)
    stream = lax.div(row, 2)
    step = lax.rem(row, 2)
    lens = lens_ref[...]
    cosine = cos_ref[...]
    sine = sin_ref[...]
    pick_all[me_s] = pick_ref[...]
    pl.semaphore_wait(barrier, n_seq - 1 + n_tensor - 1)
    sent = exchange(lambda peer: pick_ref, pick_all, pick_s, pick_r, "seq")
    for copy in sent:
        copy.wait_recv()
    embed = pick_all[0].astype(F32)
    for i in range(1, n_seq):
        embed = embed + pick_all[i].astype(F32)
    emb_all[me_t] = embed.astype(BF)
    more = exchange(lambda peer: emb_all.at[me_t], emb_all, emb_s, emb_r, "tensor")
    load_wqkv.wait()
    for load in loads:
        load.wait()
    for copy in more:
        copy.wait_recv()
    sent += more
    squares = jnp.zeros((ROWS, HD), F32)
    for i in range(n_tensor):
        part = emb_all[i].astype(F32)
        squares = squares + part * part
    norm = lax.rsqrt(jnp.sum(squares, -1, keepdims=True) / model_width + epsilon)
    normed = jnp.concatenate(
        [
            (emb_all[i].astype(F32) * norm * again_ref[:, i * HD : (i + 1) * HD]).astype(BF)
            for i in range(n_tensor)
        ],
        1,
    )
    projected = [jnp.dot(normed, wqkv[c], preferred_element_type=F32) for c in range(3)]

    def rotate(x):
        return x * cosine + pltpu.roll(x, HD // 2, 1) * sine

    queries = rotate(projected[0]).astype(BF)
    new_keys = rotate(projected[1]).astype(BF)
    new_values = projected[2].astype(BF)
    fresh_k_ref[...] = new_keys
    fresh_v_ref[...] = new_values

    inverse = HD ** (-0.5)
    load_keys.wait()
    wide_stream = lax.div(lax.broadcasted_iota(jnp.int32, (ROWS, slot_count), 0), 2)
    scores = jnp.zeros((ROWS, slot_count), F32)
    for b in range(streams):
        scores = jnp.where(wide_stream == b, nt_dot(queries, keys[b]), scores)
    scores = scores * inverse
    slot = me_s * slot_count + lax.broadcasted_iota(jnp.int32, (ROWS, slot_count), 1)
    visible = slot < lens[:, :1]
    top = jnp.max(jnp.where(visible, scores, -1e30), -1, keepdims=True)
    weights = jnp.where(visible, jnp.exp(scores - top), 0.0)
    total = jnp.sum(weights, -1, keepdims=True)
    high = weights.astype(BF)
    low = (weights - high.astype(F32)).astype(BF)
    both = jnp.concatenate([high, low], 0)
    load_values.wait()
    gathered = jnp.zeros((ROWS, HD), F32)
    for b in range(streams):
        twin = jnp.dot(both, values[b], preferred_element_type=F32)
        gathered = jnp.where(stream == b, twin[:ROWS] + twin[ROWS:], gathered)
    flash_all[me_s, :, :HD] = gathered
    flash_all[me_s, :, HD:] = jnp.where(lane < HD // 2, top, total)
    more = exchange(lambda peer: flash_all.at[me_s], flash_all, flash_s, flash_r, "seq")

    def twice(x, s):
        return jnp.where(step == s, x, pltpu.roll(x, 1 if s == 0 else ROWS - 1, 0))

    qf = queries.astype(F32)
    kf = new_keys.astype(F32)
    vf = new_values.astype(F32)
    fresh0 = jnp.sum(qf * twice(kf, 0), -1, keepdims=True) * inverse
    fresh1 = jnp.sum(qf * twice(kf, 1), -1, keepdims=True) * inverse
    second = step[:, :1] == 1
    fresh1 = jnp.where(second, fresh1, -1e30)
    fresh_top = jnp.maximum(fresh0, fresh1)
    for copy in more:
        copy.wait_recv()
    sent += more
    tops = [flash_all[i, :, HD : HD + 1] for i in range(n_seq)]
    best = fresh_top
    for item in tops:
        best = jnp.maximum(best, item)
    w0 = jnp.exp(fresh0 - best)
    w1 = jnp.where(second, jnp.exp(fresh1 - best), 0.0)
    numerator = w0 * twice(vf, 0) + w1 * twice(vf, 1)
    denominator = w0 + w1
    for i in range(n_seq):
        factor = jnp.exp(tops[i] - best)
        numerator = numerator + flash_all[i, :, :HD] * factor
        denominator = denominator + flash_all[i, :, 2 * HD - 1 : 2 * HD] * factor
    attended = (numerator / denominator).astype(BF)

    load_wout.wait()
    for i in range(n_tensor):
        mix_out[i] = jnp.dot(
            attended, wout[:, i * HD : (i + 1) * HD], preferred_element_type=F32
        )
    more = exchange(lambda peer: mix_out.at[peer], mix_all, mix_s, mix_r, "tensor")
    mix_all[me_t] = mix_out[me_t]
    for copy in more:
        copy.wait_recv()
    sent += more
    mixed = mix_all[0]
    for i in range(1, n_tensor):
        mixed = mixed + mix_all[i]
    hidden = (emb_all[me_t].astype(F32) + mixed).astype(BF)
    hidden_ref[...] = hidden
    hf = hidden.astype(F32)
    diagonal = row == lane

    def to_lanes(column):
        return jnp.sum(jnp.where(diagonal, column, 0.0), 0, keepdims=True)

    def to_rows(line, shift):
        return jnp.sum(jnp.where(lane == row + shift, line, 0.0), -1, keepdims=True)

    gated = (hf * fgain_ref[me_t]).astype(BF)

    pair = lax.rem(me_t, 2)
    group = lax.div(me_t, 2)
    partner = me_t + 1 - 2 * pair

    half = share // HALVES

    def part_logits(owner, h):
        start = pl.multiple_of(owner * share + h * half, half)
        return nt_dot(gated, table[pl.ds(start, half), :])

    pair_copies = []
    for k in range(1, groups + 1):
        g = lax.rem(group + k, groups)
        for h in range(HALVES):
            i = (k - 1) * HALVES + h
            pair_out[i] = part_logits(2 * g + 1 - pair, h).astype(BF)
            copy = pltpu.make_async_remote_copy(
                src_ref=pair_out.at[i],
                dst_ref=pair_in.at[i],
                send_sem=pair_s.at[i],
                recv_sem=pair_r.at[i],
                device_id=(me_s, partner),
                device_id_type=pl.DeviceIdType.MESH,
            )
            copy.start()
            pair_copies.append(copy)
    sq_all[me_t] = to_lanes(jnp.sum(hf * hf, -1, keepdims=True))
    sq_copies = exchange(lambda peer: sq_all.at[me_t], sq_all, sq_s, sq_r, "tensor")
    far_copies = []

    def send_far(k, h):
        g = lax.rem(group + k, groups)
        i = (k - 1) * HALVES + h
        pair_copies[i].wait_recv()
        far_out[i] = (own[i] + pair_in[i].astype(F32)).astype(BF)
        copy = pltpu.make_async_remote_copy(
            src_ref=far_out.at[i],
            dst_ref=far_in.at[i],
            send_sem=far_s.at[i],
            recv_sem=far_r.at[i],
            device_id=(me_s, 2 * g + pair),
            device_id_type=pl.DeviceIdType.MESH,
        )
        copy.start()
        far_copies.append(copy)

    for k in range(1, groups + 1):
        g = lax.rem(group + k, groups)
        for h in range(HALVES):
            own[(k - 1) * HALVES + h] = part_logits(2 * g + pair, h)
    for k in range(1, groups):
        for h in range(HALVES):
            send_far(k, h)
    for copy in sq_copies:
        copy.wait_recv()
    all_squares = sq_all[0]
    for i in range(1, n_tensor):
        all_squares = all_squares + sq_all[i]
    scale = lax.rsqrt(to_rows(all_squares, 0) / model_width + epsilon) * (
        logit_gain / math.sqrt(model_width)
    )
    stores = []
    highs = []
    for h in range(HALVES):
        i = (groups - 1) * HALVES + h
        pair_copies[i].wait_recv()
        value = own[i] + pair_in[i].astype(F32)
        for k in range(1, groups):
            far_copies[(k - 1) * HALVES + h].wait_recv()
            value = value + far_in[(k - 1) * HALVES + h].astype(F32)
        value = value * scale
        logits[h] = value
        store = pltpu.make_async_copy(
            logits.at[h], logits_hbm.at[:, pl.ds(h * half, half)], dma_sem.at[8 + h]
        )
        store.start()
        stores.append(store)
        highs.append(jnp.max(value, -1, keepdims=True))
    high_here = highs[0]
    for item in highs[1:]:
        high_here = jnp.maximum(high_here, item)
    sum_here = jnp.zeros_like(high_here)
    for h in range(HALVES):
        sum_here = sum_here + jnp.sum(jnp.exp(logits[h] - high_here), -1, keepdims=True)

    devices = n_seq * n_tensor
    me = me_s * n_tensor + me_t
    ls_all[me] = jnp.concatenate([to_lanes(high_here), to_lanes(sum_here)], 0)

    def ls_copy(k):
        peer = lax.rem(me + k, devices)
        return pltpu.make_async_remote_copy(
            src_ref=ls_all.at[me],
            dst_ref=ls_all.at[me],
            send_sem=ls_s.at[k],
            recv_sem=ls_r.at[k],
            device_id=(lax.div(peer, n_tensor), lax.rem(peer, n_tensor)),
            device_id_type=pl.DeviceIdType.MESH,
        )

    def each(action):
        def step_of(k, carry):
            action(ls_copy(k))
            return carry

        lax.fori_loop(1, devices, step_of, 0)

    each(lambda copy: copy.start())
    for copy in sent + pair_copies + sq_copies + far_copies:
        copy.wait_send()
    each(lambda copy: copy.wait_recv())
    peak = ls_all[0]
    for i in range(1, devices):
        peak = jnp.maximum(peak, ls_all[i])
    peak = peak[0:1]
    summed = jnp.zeros_like(peak)
    for i in range(devices):
        line = ls_all[i]
        summed = summed + line[1:2] * jnp.exp(line[0:1] - peak)
    lse_ref[...] = jnp.broadcast_to(to_rows(peak + jnp.log(summed), 0), (ROWS, HD))
    each(lambda copy: copy.wait_send())
    for store in stores:
        store.wait()


def close_kernel(streams, hidden_in, fresh_k, fresh_v, lse, logits, hidden_ref, newkv_ref, logp_ref):
    hidden = hidden_in[...]
    new_keys = fresh_k[...]
    new_values = fresh_v[...]
    answer = logits[...] - lse[:, :1]
    for b in range(streams):
        hidden_ref[b] = hidden[2 * b : 2 * b + 2]
        newkv_ref[0, b] = new_keys[2 * b : 2 * b + 2]
        newkv_ref[1, b] = new_values[2 * b : 2 * b + 2]
        logp_ref[b] = answer[2 * b : 2 * b + 2]


def body(
    n_seq, n_tensor,
    token_ids, cache_lengths, embed_table, attn_gain, final_gain, w_qkv, w_out, cache_keys, cache_values,
):
    streams = token_ids.shape[1]
    vocab_rows, width = embed_table.shape
    model_width = attn_gain.shape[0]
    share = vocab_rows // n_tensor
    groups = n_tensor // 2
    slot_count = cache_keys.shape[1]
    assert width == HD and 2 * streams <= ROWS and n_tensor % 2 == 0
    half = HD // 2
    powers = 10000.0 ** (-(np.arange(half, dtype=np.float64) * 2.0 / HD))
    freq = jnp.asarray(np.concatenate([powers, powers])[None].astype(np.float32))
    vmem = pl.BlockSpec(memory_space=pltpu.VMEM)
    smem = pl.BlockSpec(memory_space=pltpu.SMEM)
    hbm = pl.BlockSpec(memory_space=pl.ANY)
    sems = lambda n: pltpu.SemaphoreType.DMA((n,))
    row_shape = lambda dtype: jax.ShapeDtypeStruct((ROWS, HD), dtype)
    picked, lens, cosine, sine = pl.pallas_call(
        functools.partial(local_kernel, streams),
        out_shape=(row_shape(BF), row_shape(jnp.int32), row_shape(F32), row_shape(F32)),
        in_specs=[smem, smem, vmem, hbm],
        out_specs=(vmem,) * 4,
        scratch_shapes=[pltpu.VMEM((2 * streams, TILE, HD), BF), sems(2 * streams)],
        compiler_params=pltpu.CompilerParams(vmem_limit_bytes=60 * 1024 * 1024),
        name="rows",
    )(token_ids, cache_lengths, freq, embed_table)
    closing = pl.pallas_call(
        functools.partial(kernel, n_seq, n_tensor, streams, model_width),
        out_shape=(
            row_shape(BF),
            row_shape(BF),
            row_shape(BF),
            row_shape(F32),
            jax.ShapeDtypeStruct((ROWS, share), F32),
        ),
        in_specs=[vmem] * 6 + [hbm] * 5,
        out_specs=(vmem,) * 4 + (hbm,),
        scratch_shapes=[
            pltpu.VMEM((vocab_rows, HD), BF),
            pltpu.VMEM((3, model_width, HD), BF),
            pltpu.VMEM((HD, model_width), BF),
            pltpu.VMEM((streams, slot_count, HD), BF),
            pltpu.VMEM((streams, slot_count, HD), BF),
            pltpu.VMEM((n_seq, ROWS, HD), BF),
            pltpu.VMEM((n_tensor, ROWS, HD), BF),
            pltpu.VMEM((n_seq, ROWS, 2 * HD), F32),
            pltpu.VMEM((n_tensor, ROWS, HD), F32),
            pltpu.VMEM((n_tensor, ROWS, HD), F32),
            pltpu.VMEM((n_tensor, 1, HD), F32),
            pltpu.VMEM((n_seq * n_tensor, 2, HD), F32),
            pltpu.VMEM((groups * HALVES, ROWS, share // HALVES), BF),
            pltpu.VMEM((groups * HALVES, ROWS, share // HALVES), BF),
            pltpu.VMEM((groups * HALVES, ROWS, share // HALVES), F32),
            pltpu.VMEM((groups * HALVES, ROWS, share // HALVES), BF),
            pltpu.VMEM((groups * HALVES, ROWS, share // HALVES), BF),
            pltpu.VMEM((HALVES, ROWS, share // HALVES), F32),
            sems(8 + HALVES),
            sems(n_seq), sems(n_seq), sems(n_tensor), sems(n_tensor),
            sems(n_seq), sems(n_seq), sems(n_tensor), sems(n_tensor),
            sems(n_tensor), sems(n_tensor),
            sems(n_seq * n_tensor), sems(n_seq * n_tensor),
            sems(groups * HALVES), sems(groups * HALVES), sems(groups * HALVES), sems(groups * HALVES),
        ],
        compiler_params=pltpu.CompilerParams(
            collective_id=0, has_side_effects=True, vmem_limit_bytes=60 * 1024 * 1024
        ),
        name="decode",
    )(
        picked,
        lens,
        cosine,
        sine,
        attn_gain.reshape(1, model_width),
        final_gain.reshape(n_tensor, 1, HD),
        embed_table,
        jnp.transpose(w_qkv, (1, 0, 2)),
        w_out,
        cache_keys,
        cache_values,
    )
    hidden, new_kv, logprobs = pl.pallas_call(
        functools.partial(close_kernel, streams),
        out_shape=(
            jax.ShapeDtypeStruct((streams, 2, HD), BF),
            jax.ShapeDtypeStruct((2, streams, 2, HD), BF),
            jax.ShapeDtypeStruct((streams, 2, share), F32),
        ),
        in_specs=[vmem] * 5,
        out_specs=(vmem,) * 3,
        compiler_params=pltpu.CompilerParams(vmem_limit_bytes=60 * 1024 * 1024),
        name="close",
    )(*closing)
    return (
        jnp.transpose(hidden, (1, 0, 2)),
        jnp.transpose(new_kv, (0, 2, 1, 3)),
        jnp.transpose(logprobs, (1, 0, 2)),
    )


def solution(mesh):
    in_specs = (
        P(),
        P(),
        P("seq", "tensor"),
        P(),
        P(),
        P(None, None, "tensor"),
        P("tensor", None),
        P(None, "seq", "tensor"),
        P(None, "seq", "tensor"),
    )
    out_specs = (
        P(None, None, "tensor"),
        P(None, None, None, "tensor"),
        P(None, None, ("seq", "tensor")),
    )
    return jax.shard_map(
        functools.partial(body, mesh.shape["seq"], mesh.shape["tensor"]),
        mesh=mesh, in_specs=in_specs, out_specs=out_specs, check_vma=False,
    )
```

```python
import functools
import math

import numpy as np

import jax
import jax.numpy as jnp
from jax import lax
from jax.experimental import pallas as pl
from jax.experimental.pallas import tpu as pltpu
from jax.sharding import PartitionSpec as P

HD = 128
ROWS = 16
TILE = 16
HALVES = 2
BF = jnp.bfloat16
F32 = jnp.float32

epsilon = 1e-05
logit_gain = 2.0


def nt_dot(a, b):
    return lax.dot_general(a, b, (((1,), (1,)), ((), ())), preferred_element_type=F32)


def kernel(
    n_seq, n_tensor, streams, model_width,
    tok_ref, len_ref, freq_ref, again_ref, fgain_ref, table_hbm, wqkv_hbm, wout_hbm, keys_hbm, values_hbm,
    hidden_ref, fresh_k_ref, fresh_v_ref, lse_ref, logits_hbm,
    table, wqkv, wout, keys, values,
    pick_all, emb_all, flash_all, mix_out, mix_all, sq_all, ls_all,
    pair_out, pair_in, own, far_out, far_in, logits,
    dma_sem,
    pick_s, pick_r, emb_s, emb_r, flash_s, flash_r, mix_s, mix_r, sq_s, sq_r,
    ls_s, ls_r, pair_s, pair_r, far_s, far_r,
):
    me_s = lax.axis_index("seq")
    me_t = lax.axis_index("tensor")
    tiles = table.shape[0]
    vocab_rows = tiles * TILE
    slot_count = keys.shape[1]
    groups = n_tensor // 2
    share = vocab_rows // n_tensor

    parts = 4
    piece = tiles // parts
    loads = [
        pltpu.make_async_copy(
            table_hbm.at[pl.ds(i * piece, piece)], table.at[pl.ds(i * piece, piece)], dma_sem.at[i]
        )
        for i in range(parts)
    ]
    load_wqkv = pltpu.make_async_copy(wqkv_hbm, wqkv, dma_sem.at[parts])
    load_keys = pltpu.make_async_copy(keys_hbm, keys, dma_sem.at[parts + 1])
    load_values = pltpu.make_async_copy(values_hbm, values, dma_sem.at[parts + 2])
    load_wout = pltpu.make_async_copy(wout_hbm, wout, dma_sem.at[parts + 3])
    for load in loads + [load_wqkv, load_keys, load_values, load_wout]:
        load.start()

    def seq_peer(k):
        return lax.rem(me_s + k, n_seq)

    def tensor_peer(k):
        return lax.rem(me_t + k, n_tensor)

    barrier = pltpu.get_barrier_semaphore()
    for k in range(1, n_seq):
        pl.semaphore_signal(
            barrier, inc=1, device_id=(seq_peer(k), me_t), device_id_type=pl.DeviceIdType.MESH
        )
    for k in range(1, n_tensor):
        pl.semaphore_signal(
            barrier, inc=1, device_id=(me_s, tensor_peer(k)), device_id_type=pl.DeviceIdType.MESH
        )

    def exchange(src_of, dst, send, recv, axis):
        count = n_seq if axis == "seq" else n_tensor
        mine = me_s if axis == "seq" else me_t
        copies = []
        for k in range(1, count):
            if axis == "seq":
                peer = seq_peer(k)
                target = (peer, me_t)
            else:
                peer = tensor_peer(k)
                target = (me_s, peer)
            copy = pltpu.make_async_remote_copy(
                src_ref=src_of(peer),
                dst_ref=dst.at[mine],
                send_sem=send.at[k],
                recv_sem=recv.at[k],
                device_id=target,
                device_id_type=pl.DeviceIdType.MESH,
            )
            copy.start()
            copies.append(copy)
        return copies

    row = lax.broadcasted_iota(jnp.int32, (ROWS, HD), 0)
    lane = lax.broadcasted_iota(jnp.int32, (ROWS, HD), 1)
    stream = lax.div(row, 2)
    step = lax.rem(row, 2)
    lens = jnp.ones((ROWS, HD), jnp.int32)
    for b in range(streams):
        lens = jnp.where(stream == b, len_ref[b], lens)
    angle = (lens + step).astype(F32) * freq_ref[...]
    cosine = jnp.cos(angle)
    sine = jnp.sin(angle)
    sine = jnp.where(lane < HD // 2, -sine, sine)
    for load in loads:
        load.wait()
    picked = jnp.zeros((ROWS, HD), F32)
    for b in range(streams):
        for s in range(2):
            at = tok_ref[s, b] - me_s * vocab_rows
            tile = lax.div(jnp.minimum(jnp.maximum(at, 0), vocab_rows - 1), TILE)
            line = jnp.where(row == at - tile * TILE, table[tile].astype(F32), 0.0)
            picked = jnp.where(row == 2 * b + s, jnp.sum(line, 0, keepdims=True), picked)
    pick_all[me_s] = picked.astype(BF)
    pl.semaphore_wait(barrier, n_seq - 1 + n_tensor - 1)
    sent = exchange(lambda peer: pick_all.at[me_s], pick_all, pick_s, pick_r, "seq")
    for copy in sent:
        copy.wait_recv()
    embed = pick_all[0].astype(F32)
    for i in range(1, n_seq):
        embed = embed + pick_all[i].astype(F32)
    emb_all[me_t] = embed.astype(BF)
    more = exchange(lambda peer: emb_all.at[me_t], emb_all, emb_s, emb_r, "tensor")
    load_wqkv.wait()
    for copy in more:
        copy.wait_recv()
    sent += more
    squares = jnp.zeros((ROWS, HD), F32)
    for i in range(n_tensor):
        part = emb_all[i].astype(F32)
        squares = squares + part * part
    norm = lax.rsqrt(jnp.sum(squares, -1, keepdims=True) / model_width + epsilon)
    normed = jnp.concatenate(
        [
            (emb_all[i].astype(F32) * norm * again_ref[:, i * HD : (i + 1) * HD]).astype(BF)
            for i in range(n_tensor)
        ],
        1,
    )
    projected = [jnp.dot(normed, wqkv[c], preferred_element_type=F32) for c in range(3)]

    def rotate(x):
        return x * cosine + pltpu.roll(x, HD // 2, 1) * sine

    queries = rotate(projected[0]).astype(BF)
    new_keys = rotate(projected[1]).astype(BF)
    new_values = projected[2].astype(BF)
    fresh_k_ref[...] = new_keys
    fresh_v_ref[...] = new_values

    inverse = HD ** (-0.5)
    load_keys.wait()
    wide_stream = lax.div(lax.broadcasted_iota(jnp.int32, (ROWS, slot_count), 0), 2)
    scores = jnp.zeros((ROWS, slot_count), F32)
    for b in range(streams):
        scores = jnp.where(wide_stream == b, nt_dot(queries, keys[b]), scores)
    scores = scores * inverse
    slot = me_s * slot_count + lax.broadcasted_iota(jnp.int32, (ROWS, slot_count), 1)
    visible = slot < lens[:, :1]
    top = jnp.max(jnp.where(visible, scores, -1e30), -1, keepdims=True)
    weights = jnp.where(visible, jnp.exp(scores - top), 0.0)
    total = jnp.sum(weights, -1, keepdims=True)
    high = weights.astype(BF)
    low = (weights - high.astype(F32)).astype(BF)
    both = jnp.concatenate([high, low], 0)
    load_values.wait()
    gathered = jnp.zeros((ROWS, HD), F32)
    for b in range(streams):
        twin = jnp.dot(both, values[b], preferred_element_type=F32)
        gathered = jnp.where(stream == b, twin[:ROWS] + twin[ROWS:], gathered)
    flash_all[me_s, :, :HD] = gathered
    flash_all[me_s, :, HD:] = jnp.where(lane < HD // 2, top, total)
    more = exchange(lambda peer: flash_all.at[me_s], flash_all, flash_s, flash_r, "seq")

    def twice(x, s):
        return jnp.where(step == s, x, pltpu.roll(x, 1 if s == 0 else ROWS - 1, 0))

    qf = queries.astype(F32)
    kf = new_keys.astype(F32)
    vf = new_values.astype(F32)
    fresh0 = jnp.sum(qf * twice(kf, 0), -1, keepdims=True) * inverse
    fresh1 = jnp.sum(qf * twice(kf, 1), -1, keepdims=True) * inverse
    second = step[:, :1] == 1
    fresh1 = jnp.where(second, fresh1, -1e30)
    fresh_top = jnp.maximum(fresh0, fresh1)
    for copy in more:
        copy.wait_recv()
    sent += more
    tops = [flash_all[i, :, HD : HD + 1] for i in range(n_seq)]
    best = fresh_top
    for item in tops:
        best = jnp.maximum(best, item)
    w0 = jnp.exp(fresh0 - best)
    w1 = jnp.where(second, jnp.exp(fresh1 - best), 0.0)
    numerator = w0 * twice(vf, 0) + w1 * twice(vf, 1)
    denominator = w0 + w1
    for i in range(n_seq):
        factor = jnp.exp(tops[i] - best)
        numerator = numerator + flash_all[i, :, :HD] * factor
        denominator = denominator + flash_all[i, :, 2 * HD - 1 : 2 * HD] * factor
    attended = (numerator / denominator).astype(BF)

    load_wout.wait()
    for i in range(n_tensor):
        mix_out[i] = jnp.dot(
            attended, wout[:, i * HD : (i + 1) * HD], preferred_element_type=F32
        )
    more = exchange(lambda peer: mix_out.at[peer], mix_all, mix_s, mix_r, "tensor")
    mix_all[me_t] = mix_out[me_t]
    for copy in more:
        copy.wait_recv()
    sent += more
    mixed = mix_all[0]
    for i in range(1, n_tensor):
        mixed = mixed + mix_all[i]
    hidden = (emb_all[me_t].astype(F32) + mixed).astype(BF)
    hidden_ref[...] = hidden
    hf = hidden.astype(F32)
    diagonal = row == lane

    def to_lanes(column):
        return jnp.sum(jnp.where(diagonal, column, 0.0), 0, keepdims=True)

    def to_rows(line, shift):
        return jnp.sum(jnp.where(lane == row + shift, line, 0.0), -1, keepdims=True)

    gated = (hf * fgain_ref[me_t]).astype(BF)

    pair = lax.rem(me_t, 2)
    group = lax.div(me_t, 2)
    partner = me_t + 1 - 2 * pair

    half = share // HALVES

    def part_logits(owner, h):
        start = owner * (share // TILE) + h * (half // TILE)
        return nt_dot(gated, table[pl.ds(start, half // TILE)].reshape(half, HD))

    pair_copies = []
    for k in range(1, groups + 1):
        g = lax.rem(group + k, groups)
        for h in range(HALVES):
            i = (k - 1) * HALVES + h
            pair_out[i] = part_logits(2 * g + 1 - pair, h).astype(BF)
            copy = pltpu.make_async_remote_copy(
                src_ref=pair_out.at[i],
                dst_ref=pair_in.at[i],
                send_sem=pair_s.at[i],
                recv_sem=pair_r.at[i],
                device_id=(me_s, partner),
                device_id_type=pl.DeviceIdType.MESH,
            )
            copy.start()
            pair_copies.append(copy)
    sq_all[me_t] = to_lanes(jnp.sum(hf * hf, -1, keepdims=True))
    sq_copies = exchange(lambda peer: sq_all.at[me_t], sq_all, sq_s, sq_r, "tensor")
    far_copies = []

    def send_far(k, h):
        g = lax.rem(group + k, groups)
        i = (k - 1) * HALVES + h
        pair_copies[i].wait_recv()
        far_out[i] = (own[i] + pair_in[i].astype(F32)).astype(BF)
        copy = pltpu.make_async_remote_copy(
            src_ref=far_out.at[i],
            dst_ref=far_in.at[i],
            send_sem=far_s.at[i],
            recv_sem=far_r.at[i],
            device_id=(me_s, 2 * g + pair),
            device_id_type=pl.DeviceIdType.MESH,
        )
        copy.start()
        far_copies.append(copy)

    for k in range(1, groups + 1):
        g = lax.rem(group + k, groups)
        for h in range(HALVES):
            own[(k - 1) * HALVES + h] = part_logits(2 * g + pair, h)
    for k in range(1, groups):
        for h in range(HALVES):
            send_far(k, h)
    for copy in sq_copies:
        copy.wait_recv()
    all_squares = sq_all[0]
    for i in range(1, n_tensor):
        all_squares = all_squares + sq_all[i]
    scale = lax.rsqrt(to_rows(all_squares, 0) / model_width + epsilon) * (
        logit_gain / math.sqrt(model_width)
    )
    stores = []
    highs = []
    for h in range(HALVES):
        i = (groups - 1) * HALVES + h
        pair_copies[i].wait_recv()
        value = own[i] + pair_in[i].astype(F32)
        for k in range(1, groups):
            far_copies[(k - 1) * HALVES + h].wait_recv()
            value = value + far_in[(k - 1) * HALVES + h].astype(F32)
        value = value * scale
        logits[h] = value
        store = pltpu.make_async_copy(
            logits.at[h], logits_hbm.at[:, pl.ds(h * half, half)], dma_sem.at[8 + h]
        )
        store.start()
        stores.append(store)
        highs.append(jnp.max(value, -1, keepdims=True))
    high_here = highs[0]
    for item in highs[1:]:
        high_here = jnp.maximum(high_here, item)
    sum_here = jnp.zeros_like(high_here)
    for h in range(HALVES):
        sum_here = sum_here + jnp.sum(jnp.exp(logits[h] - high_here), -1, keepdims=True)

    devices = n_seq * n_tensor
    me = me_s * n_tensor + me_t
    ls_all[me] = jnp.concatenate([to_lanes(high_here), to_lanes(sum_here)], 0)

    def ls_copy(k):
        peer = lax.rem(me + k, devices)
        return pltpu.make_async_remote_copy(
            src_ref=ls_all.at[me],
            dst_ref=ls_all.at[me],
            send_sem=ls_s.at[k],
            recv_sem=ls_r.at[k],
            device_id=(lax.div(peer, n_tensor), lax.rem(peer, n_tensor)),
            device_id_type=pl.DeviceIdType.MESH,
        )

    def each(action):
        def step_of(k, carry):
            action(ls_copy(k))
            return carry

        lax.fori_loop(1, devices, step_of, 0)

    each(lambda copy: copy.start())
    for copy in sent + pair_copies + sq_copies + far_copies:
        copy.wait_send()
    each(lambda copy: copy.wait_recv())
    peak = ls_all[0]
    for i in range(1, devices):
        peak = jnp.maximum(peak, ls_all[i])
    peak = peak[0:1]
    summed = jnp.zeros_like(peak)
    for i in range(devices):
        line = ls_all[i]
        summed = summed + line[1:2] * jnp.exp(line[0:1] - peak)
    lse_ref[...] = jnp.broadcast_to(to_rows(peak + jnp.log(summed), 0), (ROWS, HD))
    each(lambda copy: copy.wait_send())
    for store in stores:
        store.wait()


def close_kernel(streams, hidden_in, fresh_k, fresh_v, lse, logits, hidden_ref, newkv_ref, logp_ref):
    hidden = hidden_in[...]
    new_keys = fresh_k[...]
    new_values = fresh_v[...]
    answer = logits[...] - lse[:, :1]
    for b in range(streams):
        hidden_ref[b] = hidden[2 * b : 2 * b + 2]
        newkv_ref[0, b] = new_keys[2 * b : 2 * b + 2]
        newkv_ref[1, b] = new_values[2 * b : 2 * b + 2]
        logp_ref[b] = answer[2 * b : 2 * b + 2]


def body(
    n_seq, n_tensor,
    token_ids, cache_lengths, embed_table, attn_gain, final_gain, w_qkv, w_out, cache_keys, cache_values,
):
    streams = token_ids.shape[1]
    vocab_rows, width = embed_table.shape
    model_width = attn_gain.shape[0]
    share = vocab_rows // n_tensor
    groups = n_tensor // 2
    slot_count = cache_keys.shape[1]
    assert width == HD and 2 * streams <= ROWS and n_tensor % 2 == 0
    half = HD // 2
    powers = 10000.0 ** (-(np.arange(half, dtype=np.float64) * 2.0 / HD))
    freq = jnp.asarray(np.concatenate([powers, powers])[None].astype(np.float32))
    vmem = pl.BlockSpec(memory_space=pltpu.VMEM)
    smem = pl.BlockSpec(memory_space=pltpu.SMEM)
    hbm = pl.BlockSpec(memory_space=pl.ANY)
    sems = lambda n: pltpu.SemaphoreType.DMA((n,))
    row_shape = lambda dtype: jax.ShapeDtypeStruct((ROWS, HD), dtype)
    closing = pl.pallas_call(
        functools.partial(kernel, n_seq, n_tensor, streams, model_width),
        out_shape=(
            row_shape(BF),
            row_shape(BF),
            row_shape(BF),
            row_shape(F32),
            jax.ShapeDtypeStruct((ROWS, share), F32),
        ),
        in_specs=[smem, smem, vmem, vmem, vmem] + [hbm] * 5,
        out_specs=(vmem,) * 4 + (hbm,),
        scratch_shapes=[
            pltpu.VMEM((vocab_rows // TILE, TILE, HD), BF),
            pltpu.VMEM((3, model_width, HD), BF),
            pltpu.VMEM((HD, model_width), BF),
            pltpu.VMEM((streams, slot_count, HD), BF),
            pltpu.VMEM((streams, slot_count, HD), BF),
            pltpu.VMEM((n_seq, ROWS, HD), BF),
            pltpu.VMEM((n_tensor, ROWS, HD), BF),
            pltpu.VMEM((n_seq, ROWS, 2 * HD), F32),
            pltpu.VMEM((n_tensor, ROWS, HD), F32),
            pltpu.VMEM((n_tensor, ROWS, HD), F32),
            pltpu.VMEM((n_tensor, 1, HD), F32),
            pltpu.VMEM((n_seq * n_tensor, 2, HD), F32),
            pltpu.VMEM((groups * HALVES, ROWS, share // HALVES), BF),
            pltpu.VMEM((groups * HALVES, ROWS, share // HALVES), BF),
            pltpu.VMEM((groups * HALVES, ROWS, share // HALVES), F32),
            pltpu.VMEM((groups * HALVES, ROWS, share // HALVES), BF),
            pltpu.VMEM((groups * HALVES, ROWS, share // HALVES), BF),
            pltpu.VMEM((HALVES, ROWS, share // HALVES), F32),
            sems(8 + HALVES),
            sems(n_seq), sems(n_seq), sems(n_tensor), sems(n_tensor),
            sems(n_seq), sems(n_seq), sems(n_tensor), sems(n_tensor),
            sems(n_tensor), sems(n_tensor),
            sems(n_seq * n_tensor), sems(n_seq * n_tensor),
            sems(groups * HALVES), sems(groups * HALVES), sems(groups * HALVES), sems(groups * HALVES),
        ],
        compiler_params=pltpu.CompilerParams(
            collective_id=0, has_side_effects=True, vmem_limit_bytes=60 * 1024 * 1024
        ),
        name="decode",
    )(
        token_ids,
        cache_lengths,
        freq,
        attn_gain.reshape(1, model_width),
        final_gain.reshape(n_tensor, 1, HD),
        embed_table.reshape(vocab_rows // TILE, TILE, HD),
        jnp.transpose(w_qkv, (1, 0, 2)),
        w_out,
        cache_keys,
        cache_values,
    )
    hidden, new_kv, logprobs = pl.pallas_call(
        functools.partial(close_kernel, streams),
        out_shape=(
            jax.ShapeDtypeStruct((streams, 2, HD), BF),
            jax.ShapeDtypeStruct((2, streams, 2, HD), BF),
            jax.ShapeDtypeStruct((streams, 2, share), F32),
        ),
        in_specs=[vmem] * 5,
        out_specs=(vmem,) * 3,
        compiler_params=pltpu.CompilerParams(vmem_limit_bytes=60 * 1024 * 1024),
        name="close",
    )(*closing)
    return (
        jnp.transpose(hidden, (1, 0, 2)),
        jnp.transpose(new_kv, (0, 2, 1, 3)),
        jnp.transpose(logprobs, (1, 0, 2)),
    )


def solution(mesh):
    in_specs = (
        P(),
        P(),
        P("seq", "tensor"),
        P(),
        P(),
        P(None, None, "tensor"),
        P("tensor", None),
        P(None, "seq", "tensor"),
        P(None, "seq", "tensor"),
    )
    out_specs = (
        P(None, None, "tensor"),
        P(None, None, None, "tensor"),
        P(None, None, ("seq", "tensor")),
    )
    return jax.shard_map(
        functools.partial(body, mesh.shape["seq"], mesh.shape["tensor"]),
        mesh=mesh, in_specs=in_specs, out_specs=out_specs, check_vma=False,
    )
```
